32 devices in a mesh: dp: 4 (over y, z), ep: 8 (over x, core).
Axes of the slice: x: 4, y: 2, z: 2, core: 2. Of those that a mesh axis runs over, the one named last changes fastest.
The devices are a block of a 4x4x8 slice.
Arguments:
- resid_in: bfloat16 [2, 32, 384, 2048], P(None, ('dp', 'ep')), parts along dimension 1
- expert_idx: int32 [2, 32, 384, 6], P(None, ('dp', 'ep')), parts along dimension 1
- expert_slot: int32 [2, 32, 384, 6], P(None, ('dp', 'ep')), parts along dimension 1
- w_query: bfloat16 [2048, 16, 128], replicated
- w_key: bfloat16 [2048, 16, 128], replicated
- w_value: bfloat16 [2048, 16, 128], replicated
- w_out: bfloat16 [16, 128, 2048], replicated
- w_gate: bfloat16 [2048, 2816], replicated
- w_up: bfloat16 [2048, 2816], replicated
- w_down: bfloat16 [2816, 2048], replicated
- w_router: bfloat16 [2048, 64], replicated
- norm_attn: bfloat16 [2048], replicated
- norm_ffn: bfloat16 [2048], replicated
- norm_moe: bfloat16 [2048], replicated
- expert_gate: bfloat16 [64, 2048, 1408], P('ep')
- expert_up: bfloat16 [64, 2048, 1408], P('ep')
- expert_down: bfloat16 [64, 1408, 2048], P('ep')
Outputs:
- output: bfloat16 [2, 32, 384, 2048], P(None, ('dp', 'ep')), parts along dimension 1
There are 4 independent parts. The reference program is written for one: setup_inputs(seed, part) draws one part's arguments, and reference() takes and returns one part's arrays. A program takes and returns all parts, laid end to end along the dimension named above; an argument that names none is the same for every part.
All inputs are finite; a program needn't handle non-finite values.
Results may differ from the reference program's by a relative error of at most 0.00994974.
Values are sent between devices in bfloat16 or wider.
A program may use at most 768 MiB of HBM per device.

```python
import jax
import jax.numpy as jnp
from jax import lax

D = 2048
HEADS = 16
KV_HEADS = 16
HEAD = 128
EXPERTS = 64
TOP = 6
FE = 1408
FF = 2816
SEQ = 384
SEQS = 1
GROUP = 8

TOK_MB = SEQS * SEQ
CAP = 2 * TOK_MB * TOP // EXPERTS
EPS = 1e-6
ROPE_BASE = 10000.0


def draw_device(rng_key):
    count_key, label_key, order_key = jax.random.split(rng_key, 3)
    pair_left = jax.random.randint(count_key, (EXPERTS // 2,), 0, CAP + 1)
    pair_left = pair_left.at[0].set(CAP)
    counts = jnp.stack([pair_left, CAP - pair_left], axis=1).reshape(EXPERTS)
    count_ends = jnp.cumsum(counts)
    count_starts = count_ends - counts
    copy_pos = jnp.arange(TOK_MB * TOP)
    sorted_ids = jnp.sum(copy_pos[:, None] >= count_ends[None, :], axis=1)
    slot_ranks = copy_pos - count_starts[sorted_ids]
    labels = jax.random.permutation(label_key, EXPERTS)[sorted_ids]
    token_order = jax.random.permutation(order_key, TOK_MB)
    ids_out = labels.reshape(TOP, TOK_MB).T[token_order]
    slots_out = slot_ranks.reshape(TOP, TOK_MB).T[token_order]
    return ids_out.astype(jnp.int32), slots_out.astype(jnp.int32)


def draw_routing(rng_key):
    device_keys = jax.random.split(rng_key, 2 * GROUP)
    ids_all, slots_all = jax.vmap(draw_device)(device_keys)
    return (ids_all.reshape(2, GROUP * SEQS, SEQ, TOP), slots_all.reshape(2, GROUP * SEQS, SEQ, TOP))


def setup_inputs(seed: int = 0, part: int = 0) -> dict:
    root_key = jax.random.key(seed)
    weight_keys = jax.random.split(root_key, 14)
    part_key = jax.random.fold_in(jax.random.key(seed + 1), part)
    act_key, route_key = jax.random.split(part_key)

    def normal_weight(rng_key, shape, fan_in, gain):
        raw_draw = jax.random.normal(rng_key, shape, jnp.float32)
        return (raw_draw * (gain * fan_in ** -0.5)).astype(jnp.bfloat16)

    def norm_scale(rng_key):
        return (1.0 + 0.3 * jax.random.normal(rng_key, (D,), jnp.float32)).astype(jnp.bfloat16)

    resid_in = jax.random.normal(act_key, (2, GROUP * SEQS, SEQ, D), jnp.float32).astype(jnp.bfloat16)
    expert_idx, expert_slot = draw_routing(route_key)
    return {
        'resid_in': resid_in,
        'expert_idx': expert_idx,
        'expert_slot': expert_slot,
        'w_query': normal_weight(weight_keys[0], (D, HEADS, HEAD), D, 2.0),
        'w_key': normal_weight(weight_keys[1], (D, KV_HEADS, HEAD), D, 1.0),
        'w_value': normal_weight(weight_keys[2], (D, KV_HEADS, HEAD), D, 1.0),
        'w_out': normal_weight(weight_keys[3], (HEADS, HEAD, D), HEADS * HEAD, 2.0),
        'w_gate': normal_weight(weight_keys[4], (D, FF), D, 1.0),
        'w_up': normal_weight(weight_keys[5], (D, FF), D, 1.0),
        'w_down': normal_weight(weight_keys[6], (FF, D), FF, 1.0),
        'w_router': normal_weight(weight_keys[7], (D, EXPERTS), D, 2.0),
        'norm_attn': norm_scale(weight_keys[8]),
        'norm_ffn': norm_scale(weight_keys[9]),
        'norm_moe': norm_scale(weight_keys[10]),
        'expert_gate': normal_weight(weight_keys[11], (EXPERTS, D, FE), D, 1.0),
        'expert_up': normal_weight(weight_keys[12], (EXPERTS, D, FE), D, 1.0),
        'expert_down': normal_weight(weight_keys[13], (EXPERTS, FE, D), FE, 2.0),
    }


def rms_norm(values, scale):
    widened = values.astype(jnp.float32)
    mean_sq = jnp.mean(widened * widened, axis=-1, keepdims=True)
    return (widened * lax.rsqrt(mean_sq + EPS) * scale.astype(jnp.float32)).astype(jnp.bfloat16)


def rotary(values):
    half_dim = HEAD // 2
    freqs = ROPE_BASE ** (-jnp.arange(half_dim, dtype=jnp.float32) * 2.0 / HEAD)
    angles = jnp.arange(SEQ, dtype=jnp.float32)[:, None] * freqs[None, :]
    cosine = jnp.cos(angles)[:, None, :]
    sine = jnp.sin(angles)[:, None, :]
    first = values[..., :half_dim]
    second = values[..., half_dim:]
    return jnp.concatenate([first * cosine - second * sine, second * cosine + first * sine], axis=-1)


def swiglu(normed, w_gate, w_up, w_down):
    gate_act = jnp.dot(normed, w_gate, preferred_element_type=jnp.float32)
    up_act = jnp.dot(normed, w_up, preferred_element_type=jnp.float32)
    hidden = (jax.nn.silu(gate_act) * up_act).astype(jnp.bfloat16)
    return jnp.dot(hidden, w_down, preferred_element_type=jnp.float32)


def reference(resid_in, expert_idx, expert_slot, w_query, w_key, w_value, w_out, w_gate, w_up, w_down, w_router, norm_attn, norm_ffn, norm_moe, expert_gate, expert_up, expert_down):
    group_heads = HEADS // KV_HEADS
    causal = jnp.arange(SEQ)[:, None] >= jnp.arange(SEQ)[None, :]
    query_flat = w_query.reshape(D, HEADS * HEAD)
    key_flat = w_key.reshape(D, KV_HEADS * HEAD)
    value_flat = w_value.reshape(D, KV_HEADS * HEAD)
    out_flat = w_out.reshape(HEADS * HEAD, D)

    def dense_sequence(resid):
        normed = rms_norm(resid, norm_attn)
        queries = rotary(jnp.dot(normed, query_flat, preferred_element_type=jnp.float32).reshape(SEQ, HEADS, HEAD)).astype(jnp.bfloat16)
        keys_rot = rotary(jnp.dot(normed, key_flat, preferred_element_type=jnp.float32).reshape(SEQ, KV_HEADS, HEAD)).astype(jnp.bfloat16)
        values_in = jnp.dot(normed, value_flat, preferred_element_type=jnp.float32).astype(jnp.bfloat16).reshape(SEQ, KV_HEADS, HEAD)
        keys_rep = jnp.repeat(keys_rot, group_heads, axis=1)
        values_rep = jnp.repeat(values_in, group_heads, axis=1)
        scores = jnp.einsum('qhe,khe->hqk', queries.astype(jnp.float32), keys_rep.astype(jnp.float32)) * (HEAD ** -0.5)
        probs = jax.nn.softmax(jnp.where(causal[None], scores, -1e30), axis=-1).astype(jnp.bfloat16)
        attended = jnp.einsum('hqk,khe->qhe', probs.astype(jnp.float32), values_rep.astype(jnp.float32)).astype(jnp.bfloat16)
        attn_out = jnp.dot(attended.reshape(SEQ, HEADS * HEAD), out_flat, preferred_element_type=jnp.float32)
        after_attn = (resid.astype(jnp.float32) + attn_out).astype(jnp.bfloat16)
        ffn_out = swiglu(rms_norm(after_attn, norm_ffn), w_gate, w_up, w_down)
        return after_attn.astype(jnp.float32) + ffn_out

    token_count = 2 * GROUP * TOK_MB
    dense_out = lax.map(dense_sequence, resid_in.reshape(2 * GROUP * SEQS, SEQ, D)).reshape(token_count, D)

    normed_moe = rms_norm(resid_in.reshape(token_count, D), norm_moe)
    logits = jnp.dot(normed_moe, w_router, preferred_element_type=jnp.float32)
    route_ids = expert_idx.reshape(token_count, TOP)
    route_slots = expert_slot.reshape(token_count, TOP)
    gates = jax.nn.softmax(jnp.take_along_axis(logits, route_ids, axis=1), axis=-1)
    token_pos = jnp.arange(token_count, dtype=jnp.int32)
    micro_of = token_pos // (GROUP * TOK_MB)
    device_of = (token_pos // TOK_MB) % GROUP
    buf_pos = ((route_ids * 2 + micro_of[:, None]) * GROUP + device_of[:, None]) * CAP + route_slots
    copy_count = token_count * TOP
    copy_of_row = jnp.full((EXPERTS * 2 * GROUP * CAP,), copy_count, jnp.int32)
    copy_of_row = copy_of_row.at[buf_pos.reshape(-1)].set(jnp.arange(copy_count, dtype=jnp.int32))
    copy_of_row = copy_of_row.reshape(EXPERTS, 2 * GROUP * CAP)
    gate_flat = gates.reshape(copy_count)

    def expert_step(accum_out, expert_args):
        w_a, w_b, w_c, row_copies = expert_args
        row_tokens = row_copies // TOP
        rows_in = jnp.take(normed_moe, row_tokens, axis=0, mode='fill', fill_value=0)
        expert_out = swiglu(rows_in, w_a, w_b, w_c).astype(jnp.bfloat16)
        row_gates = jnp.take(gate_flat, row_copies, mode='fill', fill_value=0)
        accum_out = accum_out.at[row_tokens].add(row_gates[:, None] * expert_out.astype(jnp.float32), mode='drop')
        return accum_out, None

    moe_out = lax.scan(expert_step, jnp.zeros((token_count, D), jnp.float32), (expert_gate, expert_up, expert_down, copy_of_row))[0]
    return (dense_out + moe_out).astype(jnp.bfloat16).reshape(2, GROUP * SEQS, SEQ, D)
```

```python
import functools

import jax
import jax.numpy as jnp
from jax import lax
from jax.experimental import pallas as pl
from jax.experimental.pallas import tpu as pltpu
from jax.sharding import PartitionSpec as P

EPS = 1e-6
ROPE_BASE = 10000.0
CAP_FACTOR = 2
CHUNK = 16
ROW_STEP = 64
VMEM_LIMIT = 63_000_000


def rms_norm(values, scale):
    widened = values.astype(jnp.float32)
    mean_sq = jnp.mean(widened * widened, axis=-1, keepdims=True)
    return (widened * lax.rsqrt(mean_sq + EPS) * scale.astype(jnp.float32)).astype(jnp.bfloat16)


def rotary(values):
    seq_len = values.shape[-3]
    head_dim = values.shape[-1]
    half_dim = head_dim // 2
    freqs = ROPE_BASE ** (-jnp.arange(half_dim, dtype=jnp.float32) * 2.0 / head_dim)
    angles = jnp.arange(seq_len, dtype=jnp.float32)[:, None] * freqs[None, :]
    cosine = jnp.cos(angles)[:, None, :]
    sine = jnp.sin(angles)[:, None, :]
    first = values[..., :half_dim]
    second = values[..., half_dim:]
    return jnp.concatenate([first * cosine - second * sine, second * cosine + first * sine], axis=-1)


def dense_branch(resid, norm_attn, w_query, w_key, w_value, w_out, norm_ffn, w_gate, w_up, w_down):
    batch, seq_len = resid.shape[0], resid.shape[1]
    heads, head_dim = w_query.shape[1], w_query.shape[2]
    kv_heads = w_key.shape[1]
    normed = rms_norm(resid, norm_attn)
    queries = rotary(jnp.einsum('bsd,dhe->bshe', normed, w_query, preferred_element_type=jnp.float32)).astype(jnp.bfloat16)
    keys_rot = rotary(jnp.einsum('bsd,dhe->bshe', normed, w_key, preferred_element_type=jnp.float32)).astype(jnp.bfloat16)
    values_in = jnp.einsum('bsd,dhe->bshe', normed, w_value, preferred_element_type=jnp.float32).astype(jnp.bfloat16)
    grouped = queries.reshape(batch, seq_len, kv_heads, heads // kv_heads, head_dim)
    scores = jnp.einsum('bqgre,bkge->bgrqk', grouped, keys_rot, preferred_element_type=jnp.float32) * (head_dim ** -0.5)
    causal = jnp.arange(seq_len)[:, None] >= jnp.arange(seq_len)[None, :]
    probs = jax.nn.softmax(jnp.where(causal, scores, -1e30), axis=-1).astype(jnp.bfloat16)
    attended = jnp.einsum('bgrqk,bkge->bqgre', probs, values_in, preferred_element_type=jnp.float32).astype(jnp.bfloat16)
    attn_out = jnp.einsum('bshe,hed->bsd', attended.reshape(batch, seq_len, heads, head_dim), w_out, preferred_element_type=jnp.float32)
    after_attn = (resid.astype(jnp.float32) + attn_out).astype(jnp.bfloat16)
    normed_ffn = rms_norm(after_attn, norm_ffn)
    gate_act = jnp.einsum('bsd,df->bsf', normed_ffn, w_gate, preferred_element_type=jnp.float32)
    up_act = jnp.einsum('bsd,df->bsf', normed_ffn, w_up, preferred_element_type=jnp.float32)
    hidden = (jax.nn.silu(gate_act) * up_act).astype(jnp.bfloat16)
    down_act = jnp.einsum('bsf,fd->bsd', hidden, w_down, preferred_element_type=jnp.float32)
    return after_attn.astype(jnp.float32) + down_act


def route_gates(tokens_in, norm_moe, w_router, route_ids):
    logits = jnp.dot(rms_norm(tokens_in, norm_moe), w_router, preferred_element_type=jnp.float32)
    hit = route_ids[:, :, None] == jnp.arange(logits.shape[1], dtype=jnp.int32)
    picked = jnp.sum(jnp.where(hit, logits[:, None, :], 0.0), axis=-1)
    return jax.nn.softmax(picked, axis=-1)


def round_up(value, step):
    return (value + step - 1) // step * step


def route_tables(ids, gates, first_expert, local_experts, cap):
    senders, tokens, _ = ids.shape
    hit = ids[..., None] == first_expert + jnp.arange(local_experts, dtype=jnp.int32)
    mask = jnp.any(hit, axis=2)
    gate = jnp.sum(jnp.where(hit, gates[..., None], 0.0), axis=2)
    before = (jnp.arange(tokens)[:, None] > jnp.arange(tokens)[None, :]).astype(jnp.bfloat16)
    rank = jnp.einsum('ut,stl->sul', before, mask.astype(jnp.bfloat16), preferred_element_type=jnp.float32).astype(jnp.int32)
    padded = round_up(jnp.sum(mask.astype(jnp.int32), axis=1), CHUNK)
    le_s = jnp.arange(senders)[:, None] > jnp.arange(senders)[None, :]
    le_e = jnp.arange(local_experts)[:, None] > jnp.arange(local_experts)[None, :]
    off_send = jnp.sum(jnp.where(le_e[None], padded[:, None, :], 0), axis=2)
    off_exp = jnp.sum(jnp.where(le_s[:, :, None], padded[None], 0), axis=1)
    send_rows = jnp.sum(padded, axis=1)
    exp_rows = jnp.sum(padded, axis=0)
    pos = jnp.where(mask, off_send[:, None, :] + rank, -1)
    cap_exp = senders * cap
    starts = jnp.arange(local_experts * cap // CHUNK, dtype=jnp.int32) * CHUNK
    inside = (starts[None, None] >= off_send[..., None]) & (starts[None, None] < (off_send + padded)[..., None])
    base = jnp.arange(local_experts, dtype=jnp.int32)[None] * cap_exp + off_exp - off_send
    chunk_row = jnp.sum(jnp.where(inside, base[..., None] + starts, 0), axis=1)
    return pos, gate, send_rows, exp_rows, chunk_row


def row_variants(limit, step):
    return list(range(step, limit, step)) + [limit]


def dispatch_kernel(rows_ref, chunk_ref, tok_ref, scale_ref, pos_ref, out_ref, stage, normed, sems, *, cap_send):
    sender = pl.program_id(0)
    count = pl.num_programs(0)
    slot = lax.rem(sender, 2)
    rows = rows_ref[sender]

    def copy(which, where, chunk):
        return pltpu.make_async_copy(
            stage.at[where, pl.ds(pl.multiple_of(chunk * CHUNK, CHUNK), CHUNK)],
            out_ref.at[pl.ds(pl.multiple_of(chunk_ref[which, chunk], CHUNK), CHUNK)],
            sems.at[where, chunk])

    def drain(which, where):
        def one(chunk, carry):
            copy(which, where, chunk).wait()
            return carry
        lax.fori_loop(0, rows_ref[which] // CHUNK, one, 0)

    @pl.when(sender >= 2)
    def _():
        drain(sender - 2, slot)

    widened = tok_ref[0].astype(jnp.float32)
    mean_sq = jnp.mean(widened * widened, axis=-1, keepdims=True)
    normed[...] = (widened * lax.rsqrt(mean_sq + EPS) * scale_ref[...].astype(jnp.float32)).astype(jnp.bfloat16)
    lower = 0
    for size in row_variants(cap_send, 128):
        @pl.when((rows > lower) & (rows <= size))
        def _(size=size):
            line = lax.broadcasted_iota(jnp.int32, (size, tok_ref.shape[1]), 0)
            chosen = line == pos_ref[0, 0:1, :]
            for expert in range(1, pos_ref.shape[1]):
                chosen = chosen | (line == pos_ref[0, expert:expert + 1, :])
            select = jnp.where(chosen, 1.0, 0.0).astype(jnp.bfloat16)

            def column(tile, inner):
                cols = pl.ds(pl.multiple_of(tile * 256, 256), 256)
                stage[slot, 0:size, cols] = jnp.dot(
                    select, normed[:, cols], preferred_element_type=jnp.float32).astype(jnp.bfloat16)
                return inner
            lax.fori_loop(0, tok_ref.shape[2] // 256, column, 0)
        lower = size

    def start(chunk, carry):
        copy(sender, slot, chunk).start()
        return carry
    lax.fori_loop(0, rows // CHUNK, start, 0)

    @pl.when(sender == count - 1)
    def _():
        @pl.when(count >= 2)
        def _():
            drain(sender - 1, 1 - slot)
        drain(sender, slot)


def dispatch(tokens, scale, pos, send_rows, chunk_row, cap_exp, local_experts):
    senders, count, width = tokens.shape
    cap_send = chunk_row.shape[1] * CHUNK
    return pl.pallas_call(
        functools.partial(dispatch_kernel, cap_send=cap_send),
        out_shape=jax.ShapeDtypeStruct((local_experts * cap_exp, width), jnp.bfloat16),
        grid_spec=pltpu.PrefetchScalarGridSpec(
            num_scalar_prefetch=2,
            grid=(senders,),
            in_specs=[
                pl.BlockSpec((1, count, width), lambda s, *_: (s, 0, 0)),
                pl.BlockSpec((1, width), lambda s, *_: (0, 0)),
                pl.BlockSpec((1, local_experts, count), lambda s, *_: (s, 0, 0)),
            ],
            out_specs=pl.BlockSpec(memory_space=pl.ANY),
            scratch_shapes=[
                pltpu.VMEM((2, cap_send, width), jnp.bfloat16),
                pltpu.VMEM((count, width), jnp.bfloat16),
                pltpu.SemaphoreType.DMA((2, cap_send // CHUNK)),
            ]),
        compiler_params=pltpu.CompilerParams(vmem_limit_bytes=VMEM_LIMIT),
        cost_estimate=pl.CostEstimate(flops=2 * senders * count * width * cap_send, bytes_accessed=senders * count * width * 6, transcendentals=0),
        name='dispatch',
    )(send_rows, chunk_row, tokens, scale.reshape(1, width), pos)


def experts_kernel(rows_ref, x_ref, gate_ref, up_ref, down_ref, y_ref, gate_buf, up_buf, down_buf, x_buf, y_buf, hid,
                   w_sems, x_sems, y_sems, *, cap_exp):
    experts = gate_ref.shape[0]
    ff = gate_ref.shape[2]
    width = gate_ref.shape[1]
    blocks = cap_exp // ROW_STEP

    def weight_copies(expert, slot):
        return (pltpu.make_async_copy(gate_ref.at[expert], gate_buf.at[slot], w_sems.at[slot, 0]),
                pltpu.make_async_copy(up_ref.at[expert], up_buf.at[slot], w_sems.at[slot, 1]),
                pltpu.make_async_copy(down_ref.at[expert], down_buf.at[slot], w_sems.at[slot, 2]))

    def x_copy(expert, slot, block):
        first = pl.multiple_of(expert * cap_exp + block * ROW_STEP, ROW_STEP)
        return pltpu.make_async_copy(x_ref.at[pl.ds(first, ROW_STEP)],
                                     x_buf.at[slot, pl.ds(pl.multiple_of(block * ROW_STEP, ROW_STEP), ROW_STEP)], x_sems.at[slot, block])

    def y_copy(expert, slot, block):
        first = pl.multiple_of(expert * cap_exp + block * ROW_STEP, ROW_STEP)
        return pltpu.make_async_copy(y_buf.at[slot, pl.ds(pl.multiple_of(block * ROW_STEP, ROW_STEP), ROW_STEP)],
                                     y_ref.at[pl.ds(first, ROW_STEP)], y_sems.at[slot, block])

    def each_block(expert, action):
        def one(block, carry):
            action(block)
            return carry
        lax.fori_loop(0, (rows_ref[expert] + ROW_STEP - 1) // ROW_STEP, one, 0)

    def fetch(expert, slot):
        each_block(expert, lambda block: x_copy(expert, slot, block).start())
        for copy in weight_copies(expert, slot):
            copy.start()

    fetch(0, 0)

    def step(expert, carry):
        slot = lax.rem(expert, 2)

        @pl.when(expert + 1 < experts)
        def _():
            fetch(expert + 1, 1 - slot)

        @pl.when(expert >= 2)
        def _():
            each_block(expert - 2, lambda block: y_copy(expert - 2, slot, block).wait())

        gate_copy, up_copy, down_copy = weight_copies(expert, slot)
        each_block(expert, lambda block: x_copy(expert, slot, block).wait())
        gate_copy.wait()
        up_copy.wait()
        rows = rows_ref[expert]
        lower = 0
        for size in row_variants(cap_exp, ROW_STEP):
            @pl.when((rows > lower) & (rows <= size))
            def _(size=size):
                def hidden(tile, inner):
                    cols = pl.ds(pl.multiple_of(tile * 128, 128), 128)
                    both = jnp.concatenate([gate_buf[slot, :, cols], up_buf[slot, :, cols]], axis=1)
                    act = jnp.dot(x_buf[slot, 0:size, :], both, preferred_element_type=jnp.float32)
                    hid[0:size, cols] = (jax.nn.silu(act[:, :128]) * act[:, 128:]).astype(jnp.bfloat16)
                    return inner
                lax.fori_loop(0, ff // 128, hidden, 0)
            lower = size
        down_copy.wait()
        lower = 0
        for size in row_variants(cap_exp, ROW_STEP):
            @pl.when((rows > lower) & (rows <= size))
            def _(size=size):
                def project(tile, inner):
                    cols = pl.ds(pl.multiple_of(tile * 256, 256), 256)
                    y_buf[slot, 0:size, cols] = jnp.dot(
                        hid[0:size, :], down_buf[slot, :, cols], preferred_element_type=jnp.float32).astype(jnp.bfloat16)
                    return inner
                lax.fori_loop(0, width // 256, project, 0)
            lower = size
        each_block(expert, lambda block: y_copy(expert, slot, block).start())
        return carry

    lax.fori_loop(0, experts, step, 0)
    for expert in range(max(experts - 2, 0), experts):
        each_block(expert, lambda block, expert=expert: y_copy(expert, expert % 2, block).wait())


def experts_call(x_rows, exp_rows, expert_gate, expert_up, expert_down):
    experts, width, ff = expert_gate.shape
    cap_exp = x_rows.shape[0] // experts
    anywhere = pl.BlockSpec(memory_space=pl.ANY)
    return pl.pallas_call(
        functools.partial(experts_kernel, cap_exp=cap_exp),
        out_shape=jax.ShapeDtypeStruct(x_rows.shape, jnp.bfloat16),
        grid_spec=pltpu.PrefetchScalarGridSpec(
            num_scalar_prefetch=1,
            grid=(1,),
            in_specs=[anywhere] * 4,
            out_specs=anywhere,
            scratch_shapes=[
                pltpu.VMEM((2, width, ff), jnp.bfloat16),
                pltpu.VMEM((2, width, ff), jnp.bfloat16),
                pltpu.VMEM((2, ff, width), jnp.bfloat16),
                pltpu.VMEM((2, cap_exp, width), jnp.bfloat16),
                pltpu.VMEM((2, cap_exp, width), jnp.bfloat16),
                pltpu.VMEM((cap_exp, ff), jnp.bfloat16),
                pltpu.SemaphoreType.DMA((2, 3)),
                pltpu.SemaphoreType.DMA((2, cap_exp // ROW_STEP)),
                pltpu.SemaphoreType.DMA((2, cap_exp // ROW_STEP)),
            ]),
        compiler_params=pltpu.CompilerParams(vmem_limit_bytes=VMEM_LIMIT),
        cost_estimate=pl.CostEstimate(flops=3 * experts * cap_exp * width * ff, bytes_accessed=6 * experts * width * ff, transcendentals=0),
        name='experts',
    )(exp_rows, x_rows, expert_gate, expert_up, expert_down)


def combine_kernel(rows_ref, chunk_ref, pos_ref, gate_ref, y_ref, out_ref, stage, parts, sems, *, cap_send):
    sender = pl.program_id(0)
    count = pl.num_programs(0)
    slot = lax.rem(sender, 2)
    rows = rows_ref[sender]

    def copy(which, where, chunk):
        return pltpu.make_async_copy(
            y_ref.at[pl.ds(pl.multiple_of(chunk_ref[which, chunk], CHUNK), CHUNK)],
            stage.at[where, pl.ds(pl.multiple_of(chunk * CHUNK, CHUNK), CHUNK)],
            sems.at[where, chunk])

    def fetch(which, where):
        def one(chunk, carry):
            copy(which, where, chunk).start()
            return carry
        lax.fori_loop(0, rows_ref[which] // CHUNK, one, 0)

    @pl.when(sender == 0)
    def _():
        stage[...] = jnp.zeros_like(stage)
        fetch(0, 0)

    @pl.when(sender + 1 < count)
    def _():
        fetch(sender + 1, 1 - slot)

    def arrive(chunk, carry):
        copy(sender, slot, chunk).wait()
        return carry
    lax.fori_loop(0, rows // CHUNK, arrive, 0)

    tokens = out_ref.shape[1]
    lower = -1
    for size in row_variants(cap_send, 256):
        @pl.when((rows > lower) & (rows <= size))
        def _(size=size):
            lane = lax.broadcasted_iota(jnp.int32, (tokens, size), 1)
            weight = jnp.zeros((tokens, size), jnp.float32)
            for expert in range(pos_ref.shape[2]):
                weight = jnp.where(lane == pos_ref[0, :, expert:expert + 1], gate_ref[0, :, expert:expert + 1], weight)
            high = weight.astype(jnp.bfloat16)
            rest = weight - high.astype(jnp.float32)
            mid = rest.astype(jnp.bfloat16)
            low = (rest - mid.astype(jnp.float32)).astype(jnp.bfloat16)
            parts[:, 0:size] = jnp.concatenate([high, mid, low], axis=0)

            def column(tile, inner):
                cols = pl.ds(pl.multiple_of(tile * 256, 256), 256)
                prod = jnp.dot(parts[:, 0:size], stage[slot, 0:size, cols], preferred_element_type=jnp.float32)
                out_ref[0, :, cols] = prod[:tokens] + (prod[tokens:2 * tokens] + prod[2 * tokens:])
                return inner
            lax.fori_loop(0, out_ref.shape[2] // 256, column, 0)
        lower = size


def combine(y_rows, pos_t, gate_t, send_rows, chunk_row):
    senders, tokens, local_experts = pos_t.shape
    width = y_rows.shape[1]
    cap_send = chunk_row.shape[1] * CHUNK
    return pl.pallas_call(
        functools.partial(combine_kernel, cap_send=cap_send),
        out_shape=jax.ShapeDtypeStruct((senders, tokens, width), jnp.float32),
        grid_spec=pltpu.PrefetchScalarGridSpec(
            num_scalar_prefetch=2,
            grid=(senders,),
            in_specs=[
                pl.BlockSpec((1, tokens, local_experts), lambda s, *_: (s, 0, 0)),
                pl.BlockSpec((1, tokens, local_experts), lambda s, *_: (s, 0, 0)),
                pl.BlockSpec(memory_space=pl.ANY),
            ],
            out_specs=pl.BlockSpec((1, tokens, width), lambda s, *_: (s, 0, 0)),
            scratch_shapes=[
                pltpu.VMEM((2, cap_send, width), jnp.bfloat16),
                pltpu.VMEM((3 * tokens, cap_send), jnp.bfloat16),
                pltpu.SemaphoreType.DMA((2, cap_send // CHUNK)),
            ]),
        compiler_params=pltpu.CompilerParams(vmem_limit_bytes=VMEM_LIMIT),
        cost_estimate=pl.CostEstimate(flops=6 * senders * tokens * width * cap_send, bytes_accessed=senders * tokens * width * 6, transcendentals=0),
        name='combine',
    )(send_rows, chunk_row, pos_t, gate_t, y_rows)


def solution(mesh):
    group_size = mesh.shape['ep']
    tok_spec = P(None, ('dp', 'ep'), None, None)
    rep_one = P(None)
    rep_two = P(None, None)
    rep_three = P(None, None, None)
    expert_spec = P('ep', None, None)

    def local_program(resid_in, expert_idx, expert_slot, w_query, w_key, w_value, w_out, w_gate, w_up, w_down, w_router, norm_attn, norm_ffn, norm_moe, expert_gate, expert_up, expert_down):
        micro_count, seqs, seq_len, width = resid_in.shape
        tokens = seqs * seq_len
        choices = expert_idx.shape[-1]
        local_experts = expert_gate.shape[0]
        capacity = CAP_FACTOR * tokens * choices // (local_experts * group_size)
        cap = round_up(capacity, CHUNK)
        flat = resid_in.reshape(micro_count, tokens, width)
        ids = expert_idx.reshape(micro_count, tokens, choices)
        gates = jax.vmap(route_gates, in_axes=(0, None, None, 0))(flat, norm_moe, w_router, ids)
        ids_all = lax.all_gather(ids, 'ep')
        gates_all = lax.all_gather(gates, 'ep')
        first = lax.axis_index('ep') * local_experts
        outputs = []
        for micro in range(micro_count):
            tokens_all = lax.all_gather(flat[micro], 'ep')
            pos, gate, send_rows, exp_rows, chunk_row = route_tables(ids_all[:, micro], gates_all[:, micro], first, local_experts, cap)
            x_rows = dispatch(tokens_all, norm_moe, pos.transpose(0, 2, 1), send_rows, chunk_row, group_size * cap, local_experts)
            y_rows = experts_call(x_rows, exp_rows, expert_gate, expert_up, expert_down)
            partial = combine(y_rows, pos, gate, send_rows, chunk_row)
            moe_out = lax.psum_scatter(partial, 'ep', scatter_dimension=0, tiled=True)
            dense_out = dense_branch(resid_in[micro], norm_attn, w_query, w_key, w_value, w_out, norm_ffn, w_gate, w_up, w_down)
            outputs.append((dense_out + moe_out.reshape(seqs, seq_len, width)).astype(jnp.bfloat16))
        return jnp.stack(outputs)

    return jax.shard_map(local_program, mesh=mesh, in_specs=(tok_spec, tok_spec, tok_spec, rep_three, rep_three, rep_three, rep_three, rep_two, rep_two, rep_two, rep_two, rep_one, rep_one, rep_one, expert_spec, expert_spec, expert_spec), out_specs=tok_spec, check_vma=False)
```

```python
import functools

import jax
import jax.numpy as jnp
from jax import lax
from jax.experimental import pallas as pl
from jax.experimental.pallas import tpu as pltpu
from jax.sharding import PartitionSpec as P

EPS = 1e-6
ROPE_BASE = 10000.0
CAP_FACTOR = 2
CHUNK = 8
ROW_STEP = 64
VMEM_LIMIT = 63_000_000
EXPERT_SIZES = (256, 320, 384, 448)
SEND_SIZES = (384,)
FF_TILE = 256
OUT_TILE = 512
DISPATCH_TILE = 2048


def rms_norm(values, scale):
    widened = values.astype(jnp.float32)
    mean_sq = jnp.mean(widened * widened, axis=-1, keepdims=True)
    return (widened * lax.rsqrt(mean_sq + EPS) * scale.astype(jnp.float32)).astype(jnp.bfloat16)


def rotary_tables(seq_len, head_dim):
    half_dim = head_dim // 2
    freqs = ROPE_BASE ** (-jnp.arange(half_dim, dtype=jnp.float32) * 2.0 / head_dim)
    angles = jnp.arange(seq_len, dtype=jnp.float32)[:, None] * freqs[None, :]
    cosine = jnp.cos(angles)
    sine = jnp.sin(angles)
    return jnp.concatenate([cosine, cosine], axis=1), jnp.concatenate([-sine, sine], axis=1)


def norm_rows(values, scale):
    widened = values.astype(jnp.float32)
    mean_sq = jnp.mean(widened * widened, axis=-1, keepdims=True)
    return (widened * lax.rsqrt(mean_sq + EPS) * scale.astype(jnp.float32)).astype(jnp.bfloat16)


def attention_kernel(resid_ref, scale_ref, cos_ref, sin_ref, wq_ref, wk_ref, wv_ref, out_ref, normed, *, head_dim):
    seqs, seq_len, width = resid_ref.shape

    @pl.when(pl.program_id(0) == 0)
    def _():
        for seq in range(seqs):
            normed[seq * seq_len:(seq + 1) * seq_len, :] = norm_rows(resid_ref[seq], scale_ref[...])

    cosine = jnp.concatenate([cos_ref[...]] * seqs, axis=0)
    sine = jnp.concatenate([sin_ref[...]] * seqs, axis=0)

    def turned(values):
        return (values * cosine + pltpu.roll(values, head_dim // 2, 1) * sine).astype(jnp.bfloat16)

    tokens_in = normed[...]
    query = jnp.dot(tokens_in, wq_ref[...], preferred_element_type=jnp.float32)
    key = jnp.dot(tokens_in, wk_ref[...], preferred_element_type=jnp.float32)
    value = jnp.dot(tokens_in, wv_ref[...], preferred_element_type=jnp.float32).astype(jnp.bfloat16)
    block = 128 if seq_len % 128 == 0 else seq_len
    for head in range(wq_ref.shape[1] // head_dim):
        cols = slice(head * head_dim, (head + 1) * head_dim)
        q_head, k_head, v_head = turned(query[:, cols]), turned(key[:, cols]), value[:, cols]
        for seq in range(seqs):
            base = seq * seq_len
            for first in range(0, seq_len, block):
                last = first + block
                scores = lax.dot_general(q_head[base + first:base + last], k_head[base:base + last], (((1,), (1,)), ((), ())),
                                         preferred_element_type=jnp.float32) * (head_dim ** -0.5)
                row = lax.broadcasted_iota(jnp.int32, (block, last), 0) + first
                scores = jnp.where(row >= lax.broadcasted_iota(jnp.int32, (block, last), 1), scores, -1e30)
                scores = jnp.exp(scores - jnp.max(scores, axis=1, keepdims=True))
                probs = (scores * (1.0 / jnp.sum(scores, axis=1, keepdims=True))).astype(jnp.bfloat16)
                out_ref[base + first:base + last, cols] = jnp.dot(
                    probs, v_head[base:base + last], preferred_element_type=jnp.float32).astype(jnp.bfloat16)


def attention(resid, scale, w_query, w_key, w_value, head_dim, first_piece, pieces):
    seqs, seq_len, width = resid.shape
    cosine, sine = rotary_tables(seq_len, head_dim)
    span = 2 * head_dim
    inner = pieces * span
    whole = lambda shape: pl.BlockSpec(shape, lambda i: (0,) * len(shape))
    piece = pl.BlockSpec((width, span), lambda i: (0, first_piece + i))
    return pl.pallas_call(
        functools.partial(attention_kernel, head_dim=head_dim),
        out_shape=jax.ShapeDtypeStruct((seqs * seq_len, inner), jnp.bfloat16),
        grid_spec=pltpu.PrefetchScalarGridSpec(
            num_scalar_prefetch=0,
            grid=(pieces,),
            in_specs=[whole(resid.shape), whole((1, width)), whole(cosine.shape), whole(sine.shape), piece, piece, piece],
            out_specs=pl.BlockSpec((seqs * seq_len, span), lambda i: (0, i)),
            scratch_shapes=[pltpu.VMEM((seqs * seq_len, width), jnp.bfloat16)]),
        compiler_params=pltpu.CompilerParams(vmem_limit_bytes=VMEM_LIMIT),
        cost_estimate=pl.CostEstimate(flops=6 * seqs * seq_len * width * inner, bytes_accessed=6 * width * inner, transcendentals=0),
        name='attention',
    )(resid, scale.reshape(1, width), cosine, sine, w_query, w_key, w_value)


def project_kernel(lhs_ref, w_ref, base_ref, out_ref):
    prod = jnp.dot(lhs_ref[...], w_ref[...], preferred_element_type=jnp.float32)
    out_ref[...] = (base_ref[...].astype(jnp.float32) + prod).astype(out_ref.dtype)


def project(lhs, weight, base, out_dtype, span, name):
    rows, depth = lhs.shape
    width = weight.shape[1]
    return pl.pallas_call(
        project_kernel,
        out_shape=jax.ShapeDtypeStruct((rows, width), out_dtype),
        grid_spec=pltpu.PrefetchScalarGridSpec(
            num_scalar_prefetch=0,
            grid=(width // span,),
            in_specs=[
                pl.BlockSpec((rows, depth), lambda i: (0, 0)),
                pl.BlockSpec((depth, span), lambda i: (0, i)),
                pl.BlockSpec((rows, span), lambda i: (0, i)),
            ],
            out_specs=pl.BlockSpec((rows, span), lambda i: (0, i))),
        compiler_params=pltpu.CompilerParams(vmem_limit_bytes=VMEM_LIMIT),
        cost_estimate=pl.CostEstimate(flops=2 * rows * depth * width, bytes_accessed=2 * depth * width + 8 * rows * width, transcendentals=0),
        name=name,
    )(lhs, weight, base)


def hidden_kernel(after_ref, scale_ref, gate_ref, up_ref, out_ref, normed):
    @pl.when(pl.program_id(0) == 0)
    def _():
        normed[...] = norm_rows(after_ref[...], scale_ref[...])

    span = gate_ref.shape[1]
    act = jnp.dot(normed[...], jnp.concatenate([gate_ref[...], up_ref[...]], axis=1), preferred_element_type=jnp.float32)
    out_ref[...] = (jax.nn.silu(act[:, :span]) * act[:, span:]).astype(jnp.bfloat16)


def hidden_call(after_attn, scale, w_gate, w_up):
    rows, width = after_attn.shape
    ff = w_gate.shape[1]
    span = 256
    return pl.pallas_call(
        hidden_kernel,
        out_shape=jax.ShapeDtypeStruct((rows, ff), jnp.bfloat16),
        grid_spec=pltpu.PrefetchScalarGridSpec(
            num_scalar_prefetch=0,
            grid=(ff // span,),
            in_specs=[
                pl.BlockSpec((rows, width), lambda i: (0, 0)),
                pl.BlockSpec((1, width), lambda i: (0, 0)),
                pl.BlockSpec((width, span), lambda i: (0, i)),
                pl.BlockSpec((width, span), lambda i: (0, i)),
            ],
            out_specs=pl.BlockSpec((rows, span), lambda i: (0, i)),
            scratch_shapes=[pltpu.VMEM((rows, width), jnp.bfloat16)]),
        compiler_params=pltpu.CompilerParams(vmem_limit_bytes=VMEM_LIMIT),
        cost_estimate=pl.CostEstimate(flops=4 * rows * width * ff, bytes_accessed=4 * width * ff, transcendentals=0),
        name='hidden',
    )(after_attn, scale.reshape(1, width), w_gate, w_up)


def dense_back(attended, resid_rows, w_out, norm_ffn, w_gate, w_up, w_down):
    width = resid_rows.shape[1]
    after_attn = project(attended, w_out.reshape(-1, width), resid_rows, jnp.bfloat16, 512, 'attn_out')
    hidden = hidden_call(after_attn, norm_ffn, w_gate, w_up)
    return project(hidden, w_down, after_attn, jnp.float32, 512, 'ffn_out')


def route_gates(normed, w_router, route_ids):
    logits = lax.dot_general(w_router, normed, (((0,), (1,)), ((), ())), preferred_element_type=jnp.float32)
    hit = route_ids[:, None, :] == jnp.arange(logits.shape[0], dtype=jnp.int32)[None, :, None]
    picked = jnp.sum(jnp.where(hit, logits[None], 0.0), axis=1)
    return jax.nn.softmax(picked, axis=0)


def round_up(value, step):
    return (value + step - 1) // step * step


def route_tables(ids, gates, first_expert, local_experts, cap):
    senders, _, tokens = ids.shape
    wanted = (first_expert + jnp.arange(local_experts, dtype=jnp.int32)).astype(ids.dtype)
    hit = ids[:, None] == wanted[None, :, None, None]
    mask = jnp.any(hit, axis=2)
    gate = jnp.sum(jnp.where(hit, gates[:, None], 0.0), axis=2)
    before = (jnp.arange(tokens)[:, None] < jnp.arange(tokens)[None, :]).astype(jnp.bfloat16)
    rank = jnp.einsum('slt,tu->slu', mask.astype(jnp.bfloat16), before, preferred_element_type=jnp.float32).astype(jnp.int32)
    padded = round_up(jnp.sum(mask.astype(jnp.int32), axis=2), CHUNK)
    le_s = jnp.arange(senders)[:, None] > jnp.arange(senders)[None, :]
    le_e = jnp.arange(local_experts)[:, None] > jnp.arange(local_experts)[None, :]
    off_send = jnp.sum(jnp.where(le_e[None], padded[:, None, :], 0), axis=2)
    off_exp = jnp.sum(jnp.where(le_s[:, :, None], padded[None], 0), axis=1)
    send_rows = jnp.sum(padded, axis=1)
    exp_rows = jnp.sum(padded, axis=0)
    pos = jnp.where(mask, off_send[:, :, None] + rank, -1)
    cap_exp = senders * cap
    starts = jnp.arange(local_experts * cap // CHUNK, dtype=jnp.int32) * CHUNK
    inside = (starts[None, None] >= off_send[..., None]) & (starts[None, None] < (off_send + padded)[..., None])
    base = jnp.arange(local_experts, dtype=jnp.int32)[None] * cap_exp + off_exp - off_send
    chunk_row = jnp.sum(jnp.where(inside, base[..., None] + starts, 0), axis=1)
    return pos, gate, send_rows, exp_rows, chunk_row


def exchange_kernel(own_ref, all_ref, send_sems, recv_sems, *, axis, size):
    me = lax.axis_index(axis)
    barrier = pltpu.get_barrier_semaphore()
    for step in range(1, size):
        pl.semaphore_signal(barrier, inc=1, device_id={axis: lax.rem(me + step, size)}, device_id_type=pl.DeviceIdType.MESH)
    pl.semaphore_wait(barrier, size - 1)
    copies = []
    for step in range(1, size):
        copy = pltpu.make_async_remote_copy(
            src_ref=own_ref, dst_ref=all_ref.at[me], send_sem=send_sems.at[step - 1], recv_sem=recv_sems.at[step - 1],
            device_id={axis: lax.rem(me + step, size)}, device_id_type=pl.DeviceIdType.MESH)
        copy.start()
        copies.append(copy)
    all_ref[me] = own_ref[...]
    for copy in copies:
        copy.wait()


def exchange(own, axis, size):
    vmem = pl.BlockSpec(memory_space=pltpu.VMEM)
    return pl.pallas_call(
        functools.partial(exchange_kernel, axis=axis, size=size),
        out_shape=jax.ShapeDtypeStruct((size,) + own.shape, own.dtype),
        in_specs=[vmem],
        out_specs=vmem,
        scratch_shapes=[pltpu.SemaphoreType.DMA((size - 1,)), pltpu.SemaphoreType.DMA((size - 1,))],
        compiler_params=pltpu.CompilerParams(collective_id=0, has_side_effects=True),
        cost_estimate=pl.CostEstimate(flops=10_000_000, bytes_accessed=own.size * 64, transcendentals=0),
        name='exchange',
    )(own)


def row_variants(limit, sizes):
    return [size for size in sizes if size < limit] + [limit]


def dispatch_kernel(rows_ref, chunk_ref, tok_ref, pos_ref, out_ref, stage, sems, *, cap_send):
    sender = pl.program_id(0)
    count = pl.num_programs(0)
    slot = lax.rem(sender, 2)
    rows = rows_ref[sender]

    def copy(which, where, chunk):
        return pltpu.make_async_copy(
            stage.at[where, pl.ds(pl.multiple_of(chunk * CHUNK, CHUNK), CHUNK)],
            out_ref.at[pl.ds(pl.multiple_of(chunk_ref[which, chunk], CHUNK), CHUNK)],
            sems.at[where, chunk])

    def drain(which, where):
        def one(chunk, carry):
            copy(which, where, chunk).wait()
            return carry
        lax.fori_loop(0, rows_ref[which] // CHUNK, one, 0)

    @pl.when(sender >= 2)
    def _():
        drain(sender - 2, slot)

    lower = 0
    for size in row_variants(cap_send, SEND_SIZES):
        @pl.when((rows > lower) & (rows <= size))
        def _(size=size):
            line = lax.broadcasted_iota(jnp.int32, (size, tok_ref.shape[1]), 0)
            chosen = line == pos_ref[0, 0:1, :]
            for expert in range(1, pos_ref.shape[1]):
                chosen = chosen | (line == pos_ref[0, expert:expert + 1, :])
            select = jnp.where(chosen, 1.0, 0.0).astype(jnp.bfloat16)

            def column(tile, inner):
                cols = pl.ds(pl.multiple_of(tile * DISPATCH_TILE, DISPATCH_TILE), DISPATCH_TILE)
                stage[slot, 0:size, cols] = jnp.dot(
                    select, tok_ref[0, :, cols], preferred_element_type=jnp.float32).astype(jnp.bfloat16)
                return inner
            lax.fori_loop(0, tok_ref.shape[2] // DISPATCH_TILE, column, 0)
        lower = size

    def start(chunk, carry):
        copy(sender, slot, chunk).start()
        return carry
    lax.fori_loop(0, rows // CHUNK, start, 0)

    @pl.when(sender == count - 1)
    def _():
        @pl.when(count >= 2)
        def _():
            drain(sender - 1, 1 - slot)
        drain(sender, slot)


def dispatch(tokens, pos, send_rows, chunk_row, cap_exp, local_experts):
    senders, count, width = tokens.shape
    cap_send = chunk_row.shape[1] * CHUNK
    return pl.pallas_call(
        functools.partial(dispatch_kernel, cap_send=cap_send),
        out_shape=jax.ShapeDtypeStruct((local_experts * cap_exp, width), jnp.bfloat16),
        grid_spec=pltpu.PrefetchScalarGridSpec(
            num_scalar_prefetch=2,
            grid=(senders,),
            in_specs=[
                pl.BlockSpec((1, count, width), lambda s, *_: (s, 0, 0)),
                pl.BlockSpec((1, local_experts, count), lambda s, *_: (s, 0, 0)),
            ],
            out_specs=pl.BlockSpec(memory_space=pl.ANY),
            scratch_shapes=[
                pltpu.VMEM((2, cap_send, width), jnp.bfloat16),
                pltpu.SemaphoreType.DMA((2, cap_send // CHUNK)),
            ]),
        compiler_params=pltpu.CompilerParams(vmem_limit_bytes=VMEM_LIMIT),
        cost_estimate=pl.CostEstimate(flops=2 * senders * count * width * cap_send, bytes_accessed=senders * count * width * 6, transcendentals=0),
        name='dispatch',
    )(send_rows, chunk_row, tokens, pos)


def experts_kernel(rows_ref, x_ref, gate_ref, up_ref, down_ref, y_ref, gate_buf, up_buf, down_buf, x_buf, y_buf, hid, act_a, act_b,
                   w_sems, x_sems, y_sems, *, cap_exp):
    experts = gate_ref.shape[0]
    ff = gate_ref.shape[2]
    width = gate_ref.shape[1]
    blocks = cap_exp // ROW_STEP

    def weight_copies(expert, slot):
        return (pltpu.make_async_copy(gate_ref.at[expert], gate_buf.at[slot], w_sems.at[slot, 0]),
                pltpu.make_async_copy(up_ref.at[expert], up_buf.at[slot], w_sems.at[slot, 1]),
                pltpu.make_async_copy(down_ref.at[expert], down_buf.at[slot], w_sems.at[slot, 2]))

    def x_copy(expert, slot, block):
        first = pl.multiple_of(expert * cap_exp + block * ROW_STEP, ROW_STEP)
        return pltpu.make_async_copy(x_ref.at[pl.ds(first, ROW_STEP)],
                                     x_buf.at[slot, pl.ds(pl.multiple_of(block * ROW_STEP, ROW_STEP), ROW_STEP)], x_sems.at[slot, block])

    def y_copy(expert, slot, block):
        first = pl.multiple_of(expert * cap_exp + block * ROW_STEP, ROW_STEP)
        return pltpu.make_async_copy(y_buf.at[slot, pl.ds(pl.multiple_of(block * ROW_STEP, ROW_STEP), ROW_STEP)],
                                     y_ref.at[pl.ds(first, ROW_STEP)], y_sems.at[slot, block])

    def each_block(expert, action):
        def one(block, carry):
            action(block)
            return carry
        lax.fori_loop(0, (rows_ref[expert] + ROW_STEP - 1) // ROW_STEP, one, 0)

    def fetch(expert, slot):
        each_block(expert, lambda block: x_copy(expert, slot, block).start())
        for copy in weight_copies(expert, slot):
            copy.start()

    fetch(0, 0)

    def step(expert, carry):
        slot = lax.rem(expert, 2)

        @pl.when(expert + 1 < experts)
        def _():
            fetch(expert + 1, 1 - slot)

        @pl.when(expert >= 2)
        def _():
            each_block(expert - 2, lambda block: y_copy(expert - 2, slot, block).wait())

        gate_copy, up_copy, down_copy = weight_copies(expert, slot)
        each_block(expert, lambda block: x_copy(expert, slot, block).wait())
        gate_copy.wait()
        up_copy.wait()
        rows = rows_ref[expert]
        lower = 0
        for size in row_variants(cap_exp, EXPERT_SIZES):
            @pl.when((rows > lower) & (rows <= size))
            def _(size=size):
                def gate_up(first, span, act):
                    cols = pl.ds(first, span)
                    both = jnp.concatenate([gate_buf[slot, :, cols], up_buf[slot, :, cols]], axis=1)
                    act[0:size, 0:2 * span] = jnp.dot(x_buf[slot, 0:size, :], both, preferred_element_type=jnp.float32)

                def glue(first, span, act):
                    hid[0:size, pl.ds(first, span)] = (
                        jax.nn.silu(act[0:size, 0:span]) * act[0:size, span:2 * span]).astype(jnp.bfloat16)

                def at(tile):
                    return tile * FF_TILE if isinstance(tile, int) else pl.multiple_of(tile * FF_TILE, FF_TILE)

                def pair(index, inner):
                    gate_up(at(2 * index + 1), FF_TILE, act_b)
                    glue(at(2 * index), FF_TILE, act_a)
                    gate_up(at(2 * index + 2), FF_TILE, act_a)
                    glue(at(2 * index + 1), FF_TILE, act_b)
                    return inner
                whole = ff // FF_TILE
                rest = ff % FF_TILE
                gate_up(0, FF_TILE, act_a)
                lax.fori_loop(0, (whole - 1) // 2, pair, 0)
                done = 2 * ((whole - 1) // 2) + 1
                tail = [(at(tile), FF_TILE) for tile in range(done, whole)] + ([(whole * FF_TILE, rest)] if rest else [])
                held, free = (at(done - 1), FF_TILE, act_a), act_b
                for first, span in tail:
                    gate_up(first, span, free)
                    glue(*held)
                    held, free = (first, span, free), held[2]
                glue(*held)
            lower = size
        down_copy.wait()
        lower = 0
        for size in row_variants(cap_exp, EXPERT_SIZES):
            @pl.when((rows > lower) & (rows <= size))
            def _(size=size):
                def project(tile, inner):
                    cols = pl.ds(pl.multiple_of(tile * OUT_TILE, OUT_TILE), OUT_TILE)
                    y_buf[slot, 0:size, cols] = jnp.dot(
                        hid[0:size, :], down_buf[slot, :, cols], preferred_element_type=jnp.float32).astype(jnp.bfloat16)
                    return inner
                lax.fori_loop(0, width // OUT_TILE, project, 0)
            lower = size
        each_block(expert, lambda block: y_copy(expert, slot, block).start())
        return carry

    lax.fori_loop(0, experts, step, 0)
    for expert in range(max(experts - 2, 0), experts):
        each_block(expert, lambda block, expert=expert: y_copy(expert, expert % 2, block).wait())


def experts_call(x_rows, exp_rows, expert_gate, expert_up, expert_down):
    experts, width, ff = expert_gate.shape
    cap_exp = x_rows.shape[0] // experts
    anywhere = pl.BlockSpec(memory_space=pl.ANY)
    return pl.pallas_call(
        functools.partial(experts_kernel, cap_exp=cap_exp),
        out_shape=jax.ShapeDtypeStruct(x_rows.shape, jnp.bfloat16),
        grid_spec=pltpu.PrefetchScalarGridSpec(
            num_scalar_prefetch=1,
            grid=(1,),
            in_specs=[anywhere] * 4,
            out_specs=anywhere,
            scratch_shapes=[
                pltpu.VMEM((2, width, ff), jnp.bfloat16),
                pltpu.VMEM((2, width, ff), jnp.bfloat16),
                pltpu.VMEM((2, ff, width), jnp.bfloat16),
                pltpu.VMEM((2, cap_exp, width), jnp.bfloat16),
                pltpu.VMEM((2, cap_exp, width), jnp.bfloat16),
                pltpu.VMEM((cap_exp, ff), jnp.bfloat16),
                pltpu.VMEM((cap_exp, 2 * FF_TILE), jnp.float32),
                pltpu.VMEM((cap_exp, 2 * FF_TILE), jnp.float32),
                pltpu.SemaphoreType.DMA((2, 3)),
                pltpu.SemaphoreType.DMA((2, cap_exp // ROW_STEP)),
                pltpu.SemaphoreType.DMA((2, cap_exp // ROW_STEP)),
            ]),
        compiler_params=pltpu.CompilerParams(vmem_limit_bytes=VMEM_LIMIT),
        cost_estimate=pl.CostEstimate(flops=3 * experts * cap_exp * width * ff, bytes_accessed=6 * experts * width * ff, transcendentals=0),
        name='experts',
    )(exp_rows, x_rows, expert_gate, expert_up, expert_down)


def combine_kernel(rows_ref, chunk_ref, pos_ref, gate_ref, next_pos_ref, next_gate_ref, y_ref, out_ref,
                   stage_a, stage_b, parts_a, parts_b, sems, *, cap):
    step = pl.program_id(0)
    steps = pl.num_programs(0)
    tokens = out_ref.shape[1]
    stages = (stage_a, stage_b)
    parts = (parts_a, parts_b)

    def copy(sender, side, chunk):
        return pltpu.make_async_copy(
            y_ref.at[pl.ds(pl.multiple_of(chunk_ref[sender, chunk], CHUNK), CHUNK)],
            stages[side].at[pl.ds(pl.multiple_of(chunk * CHUNK, CHUNK), CHUNK)],
            sems.at[side, chunk])

    def each_chunk(sender, action):
        def one(chunk, carry):
            action(chunk)
            return carry
        lax.fori_loop(0, rows_ref[sender] // CHUNK, one, 0)

    def fetch(sender, side):
        each_chunk(sender, lambda chunk: copy(sender, side, chunk).start())

    def build(pos, gate, into):
        lane = lax.broadcasted_iota(jnp.int32, (tokens, cap), 1).astype(jnp.float32)
        where_row = jnp.transpose(pos.astype(jnp.float32))
        gate_row = jnp.transpose(gate)
        weight = jnp.zeros((tokens, cap), jnp.float32)
        for expert in range(pos.shape[0]):
            weight = jnp.where(lane == where_row[:, expert:expert + 1], gate_row[:, expert:expert + 1], weight)
        high = weight.astype(jnp.bfloat16)
        rest = weight - high.astype(jnp.float32)
        mid = rest.astype(jnp.bfloat16)
        into[:, 0:cap] = high
        into[:, cap:2 * cap] = mid
        into[:, 2 * cap:3 * cap] = (rest - mid.astype(jnp.float32)).astype(jnp.bfloat16)

    @pl.when(step == 0)
    def _():
        stage_a[...] = jnp.zeros_like(stage_a)
        stage_b[...] = jnp.zeros_like(stage_b)
        fetch(0, 0)
        build(pos_ref[0], gate_ref[0], parts_a)

    for side in range(2):
        sender = 2 * step + side
        if side == 0:
            fetch(sender + 1, 1)
        else:
            @pl.when(step + 1 < steps)
            def _():
                fetch(sender + 1, 0)
        each_chunk(sender, lambda chunk: copy(sender, side, chunk).wait())
        rows = rows_ref[sender]
        lower = -1
        for size in row_variants(cap, SEND_SIZES):
            @pl.when((rows > lower) & (rows <= size))
            def _(size=size):
                lhs = jnp.concatenate([parts[side][:, part * cap:part * cap + size] for part in range(3)], axis=1)
                rhs = jnp.concatenate([stages[side][0:size, :]] * 3, axis=0)
                out_ref[side] = jnp.dot(lhs, rhs, preferred_element_type=jnp.float32)
                if side == 0:
                    build(pos_ref[1], gate_ref[1], parts_b)
                else:
                    build(next_pos_ref[0], next_gate_ref[0], parts_a)
            lower = size


def combine(y_rows, pos, gate, send_rows, chunk_row):
    senders, local_experts, tokens = pos.shape
    width = y_rows.shape[1]
    chunks = chunk_row.shape[1]
    cap = round_up(chunks * CHUNK, 128)
    table = pl.BlockSpec((2, local_experts, tokens), lambda s, *_: (s, 0, 0))
    ahead = pl.BlockSpec((2, local_experts, tokens), lambda s, *_: (jnp.minimum(s + 1, senders // 2 - 1), 0, 0))
    return pl.pallas_call(
        functools.partial(combine_kernel, cap=cap),
        out_shape=jax.ShapeDtypeStruct((senders, tokens, width), jnp.float32),
        grid_spec=pltpu.PrefetchScalarGridSpec(
            num_scalar_prefetch=2,
            grid=(senders // 2,),
            in_specs=[table, table, ahead, ahead, pl.BlockSpec(memory_space=pl.ANY)],
            out_specs=pl.BlockSpec((2, tokens, width), lambda s, *_: (s, 0, 0)),
            scratch_shapes=[
                pltpu.VMEM((cap, width), jnp.bfloat16),
                pltpu.VMEM((cap, width), jnp.bfloat16),
                pltpu.VMEM((tokens, 3 * cap), jnp.bfloat16),
                pltpu.VMEM((tokens, 3 * cap), jnp.bfloat16),
                pltpu.SemaphoreType.DMA((2, chunks)),
            ]),
        compiler_params=pltpu.CompilerParams(vmem_limit_bytes=VMEM_LIMIT),
        cost_estimate=pl.CostEstimate(flops=6 * senders * tokens * width * cap, bytes_accessed=senders * tokens * width * 6, transcendentals=0),
        name='combine',
    )(send_rows, chunk_row, pos, gate, pos, gate, y_rows)


def solution(mesh):
    group_size = mesh.shape['ep']
    tok_spec = P(None, ('dp', 'ep'), None, None)
    rep_one = P(None)
    rep_two = P(None, None)
    rep_three = P(None, None, None)
    expert_spec = P('ep', None, None)

    def local_program(resid_in, expert_idx, expert_slot, w_query, w_key, w_value, w_out, w_gate, w_up, w_down, w_router, norm_attn, norm_ffn, norm_moe, expert_gate, expert_up, expert_down):
        micro_count, seqs, seq_len, width = resid_in.shape
        tokens = seqs * seq_len
        choices = expert_idx.shape[-1]
        local_experts = expert_gate.shape[0]
        capacity = CAP_FACTOR * tokens * choices // (local_experts * group_size)
        cap = round_up(capacity, CHUNK)
        flat = resid_in.reshape(micro_count, tokens, width)
        normed = [rms_norm(flat[micro], norm_moe) for micro in range(micro_count)]
        ids = expert_idx.reshape(micro_count, tokens, choices).transpose(0, 2, 1)
        gates = jnp.stack([route_gates(normed[micro], w_router, ids[micro]) for micro in range(micro_count)])
        routes = exchange(jnp.concatenate([ids.astype(jnp.float32), gates], axis=1), 'ep', group_size)
        first = lax.axis_index('ep') * local_experts
        tables = jax.vmap(lambda r: route_tables(r[:, :choices], r[:, choices:], first, local_experts, cap), in_axes=1)(routes)

        resid_rows = resid_in.reshape(micro_count * tokens, width)
        resid_seqs = resid_in.reshape(micro_count * seqs, seq_len, width)
        head_dim = w_query.shape[2]
        w_qkv = [weight.reshape(width, -1) for weight in (w_query, w_key, w_value)]
        pieces = w_qkv[0].shape[1] // (2 * head_dim)
        partials = []
        for micro in range(micro_count):
            tokens_all = lax.all_gather(normed[micro], 'ep')
            pos, gate, send_rows, exp_rows, chunk_row = [table[micro] for table in tables]
            if micro == 0:
                pos, w_qkv = lax.optimization_barrier((pos, w_qkv))
            else:
                pos = lax.optimization_barrier((pos, partials[-1]))[0]
            x_rows = dispatch(tokens_all, pos, send_rows, chunk_row, group_size * cap, local_experts)
            y_rows = experts_call(x_rows, exp_rows, expert_gate, expert_up, expert_down)
            partials.append(combine(y_rows, pos, gate, send_rows, chunk_row))
        w_late = lax.optimization_barrier((w_qkv, partials[-1]))[0]
        attended = attention(resid_seqs, norm_attn, *w_late, head_dim, 0, pieces)
        dense_out = dense_back(attended, resid_rows, w_out, norm_ffn, w_gate, w_up, w_down).reshape(resid_in.shape)
        outputs = []
        for micro in range(micro_count):
            moe_out = lax.psum_scatter(partials[micro], 'ep', scatter_dimension=0, tiled=True).reshape(seqs, seq_len, width)
            outputs.append((dense_out[micro] + moe_out).astype(jnp.bfloat16))
        return jnp.stack(outputs)

    return jax.shard_map(local_program, mesh=mesh, in_specs=(tok_spec, tok_spec, tok_spec, rep_three, rep_three, rep_three, rep_three, rep_two, rep_two, rep_two, rep_two, rep_one, rep_one, rep_one, expert_spec, expert_spec, expert_spec), out_specs=tok_spec, check_vma=False)
```
